256 devices in a mesh: rows: 32 (over x, y, core), feat: 8 (over z).
Axes of the slice: x: 4, y: 4, z: 8, core: 2. Of those that a mesh axis runs over, the one named last changes fastest.
Arguments:
- queries: bfloat16 [196608, 4096], P('rows', 'feat'), may hold values from -6 to 6
- projection: bfloat16 [4096, 128], P('feat'), may hold values from -0.09375 to 0.09375
- models: float32 [64, 128], replicated, may hold values from -0.5 to 0.5
- first: int32 [196608], P('rows'), may hold values from 0 to 63
- second: int32 [196608], P('rows'), may hold values from 0 to 63
- wins: int32 [196608], P('rows'), may hold values 0 or 1
Outputs:
- update_proj: float32 [4096, 128], P('feat')
- update_models: float32 [64, 128], replicated
- loss: float32 [], replicated
The draws below stay inside these ranges and needn't reach their ends.
All inputs are finite; a program needn't handle non-finite values. No bound on the sum of `wins` on one device may be relied on, other than what follows from the above.
Results may differ from the reference program's by a relative error of at most 0.00045.
The reference program's roundings to bfloat16 on the way (of `back`) count: a program that leaves them out, or rounds other values in their place, can miss the bound.
Values may be sent and summed in bfloat16 or wider, within the bound.
No kernel may reach another device: no remote copies, remote signals or barrier semaphores. Data moves between devices by JAX's collectives and lax.ppermute only.
A program may use at most 64 MiB of HBM per device.

```python
import jax
import jax.numpy as jnp
from jax import lax

D = 4096
R = 128
NM = 64
TOKENS = 196608


def touch_ends(array, own_key, smallest, high):
    longest = array.shape.index(max(array.shape))
    spots = []
    for shift in (0, 1):
        where = [jax.random.randint(jax.random.fold_in(own_key, axis), (), 0, length) for axis, length in enumerate(array.shape)]
        where[longest] = (where[longest] + shift) % array.shape[longest]
        spots.append(tuple(where))
    return array.at[spots[0]].set(smallest).at[spots[1]].set(high)


def levels(stream_key, dims, cuts, low, largest):
    gain, own = 1.0, jax.random.fold_in(stream_key, 6)
    for axis_at, blocks in cuts:
        draws = jnp.exp(jax.random.uniform(jax.random.fold_in(own, axis_at), (blocks,), jnp.float32, low / len(cuts), largest / len(cuts)))
        gain = gain * jnp.repeat(draws, dims[axis_at] // blocks).reshape([-1 if axis == axis_at else 1 for axis in range(len(dims))])
    return gain


def scatter_about(own_key, shape, scale, limit, split=(), kind=jnp.bfloat16):
    entries = jax.random.normal(own_key, shape, jnp.float32) * scale
    if len(split) > 0:
        entries = levels(own_key, shape, split, -0.22, 0.18) * entries
    return jnp.clip(entries, min=-limit, max=limit).astype(kind)


def setup_inputs(seed: int = 0) -> dict:
    keys = jax.random.split(jax.random.key(seed), 7)
    queries = scatter_about(keys[0], (TOKENS, D), 1.0, 6.0, ((0, 32), (1, 8)))
    projection = scatter_about(keys[1], (D, R), D ** -0.5, 0.09375, ((0, 8),))
    models = scatter_about(keys[2], (NM, R), R ** -0.5, 0.5, (), jnp.float32)
    first = touch_ends(jax.random.randint(keys[3], (TOKENS,), 0, NM), jax.random.fold_in(keys[3], 1), 0, NM - 1).astype(jnp.int32)
    second = touch_ends(jax.random.randint(keys[4], (TOKENS,), 0, NM), jax.random.fold_in(keys[4], 1), 0, NM - 1).astype(jnp.int32)
    wins = touch_ends((jax.random.randint(keys[5], (TOKENS,), 0, 2) < 1).astype(jnp.int32), jax.random.fold_in(keys[5], 1), 0, 1)
    return {"queries": queries, "projection": projection, "models": models, "first": first, "second": second, "wins": wins}


def reference(queries, projection, models, first, second, wins):
    routed = jnp.dot(queries, projection, preferred_element_type=jnp.float32)
    gap = jnp.take(models, first, axis=0) - jnp.take(models, second, axis=0)
    margin = lax.optimization_barrier(jnp.sum(routed * gap, axis=-1))
    sign = 2.0 * wins.astype(jnp.float32) - 1.0
    loss = jnp.sum(jax.nn.softplus(-sign * margin)) / TOKENS
    coef = -sign * jax.nn.sigmoid(-sign * margin) / TOKENS
    back = (coef[:, None] * gap).astype(jnp.bfloat16)
    grad_proj = jnp.dot(queries.T, back, preferred_element_type=jnp.float32)
    labels = jnp.arange(NM, dtype=jnp.int32)[:, None]
    pick = (labels == first[None, :]).astype(jnp.float32) - (labels == second[None, :]).astype(jnp.float32)
    grad_models = jnp.dot(pick, coef[:, None] * routed, precision=lax.Precision.HIGHEST)
    total = jnp.sum(grad_proj * grad_proj) + jnp.sum(grad_models * grad_models)
    scale = jnp.sqrt(jnp.float32(D * R + NM * R)) / (jnp.sqrt(total) + 1e-06)
    return (scale * grad_proj, scale * grad_models, loss)
```

```python
import functools

import jax
import jax.numpy as jnp
from jax import lax
from jax.experimental import pallas as pl
from jax.experimental.pallas import tpu as pltpu
from jax.sharding import Mesh
from jax.sharding import PartitionSpec as P

D = 4096
R = 128
NM = 64
LANES = 128
ROWS = ("rows_0", "rows_1", "rows_2")
F32 = jnp.float32
BF16 = jnp.bfloat16
MIB = 1 << 20
CHUNK = 1024


def exchange(x, axis):
    return lax.all_to_all(x, axis, split_axis=0, concat_axis=0, tiled=True)


def pieces(x, count):
    terms = []
    for _ in range(count):
        term = x.astype(BF16)
        terms.append(term)
        x = x - term.astype(F32)
    return terms


def contract(a, b, dim_a, dim_b):
    return lax.dot_general(a, b, (((dim_a,), (dim_b,)), ((), ())), preferred_element_type=F32)


def model_table(models):
    stacked = jnp.concatenate([term.astype(F32) for term in pieces(models, 3)], axis=0)
    return stacked.T.astype(BF16)


def picks(first_ref, second_ref, start, count):
    labels = lax.broadcasted_iota(jnp.int32, (NM, LANES), 0)
    tiles = []
    for i in range(start // LANES, (start + count) // LANES):
        one = jnp.where(labels == first_ref[i : i + 1, :], 1.0, 0.0)
        two = jnp.where(labels == second_ref[i : i + 1, :], 1.0, 0.0)
        tiles.append(one - two)
    return jnp.concatenate(tiles, axis=1)


def gaps(table, pick):
    pick = pick.astype(BF16)
    return contract(table, jnp.concatenate([pick, pick, pick], axis=0), 1, 0)


def margin_kernel(first_ref, second_ref, models_ref, proj_ref, q_hbm, out_ref, q_ref, sems):
    tokens = q_hbm.shape[0]
    copies = []
    for i in range(tokens // CHUNK):
        rows = pl.ds(i * CHUNK, CHUNK)
        copies.append(pltpu.make_async_copy(q_hbm.at[rows, :], q_ref.at[rows, :], sems.at[i]))
        copies[-1].start()
    table = model_table(models_ref[...])
    proj = proj_ref[...].astype(F32).T.astype(BF16)
    for i in range(tokens // CHUNK):
        gap = gaps(table, picks(first_ref, second_ref, i * CHUNK, CHUNK))
        copies[i].wait()
        routed = contract(proj, q_ref[pl.ds(i * CHUNK, CHUNK), :], 1, 1)
        margin = jnp.sum(routed * gap, axis=0, keepdims=True)
        for j in range(CHUNK // LANES):
            row = margin[:, j * LANES : (j + 1) * LANES]
            for k in range(out_ref.shape[0]):
                out_ref[k, pl.ds(i * (CHUNK // LANES) + j, 1), :] = row


def grad_kernel(total, share, margins_ref, first_ref, second_ref, wins_ref, models_ref, proj_ref, q_ref, out_ref, loss_ref, coef_ref, acc_ref):
    tokens = q_ref.shape[0]
    margin = margins_ref[0]
    for k in range(1, margins_ref.shape[0]):
        margin = margin + margins_ref[k]
    sign = 2.0 * wins_ref[...].astype(F32) - 1.0
    wrong = -sign * margin
    loss_ref[...] = jax.nn.softplus(wrong) / total
    coef_ref[...] = -sign * jax.nn.sigmoid(wrong) / total
    table = model_table(models_ref[...])
    for i in range(tokens // CHUNK):
        pick = picks(first_ref, second_ref, i * CHUNK, CHUNK)
        gap = gaps(table, pick)
        first_row = i * CHUNK // LANES
        coef = jnp.concatenate([coef_ref[first_row + j : first_row + j + 1, :] for j in range(CHUNK // LANES)], axis=1)
        left = jnp.concatenate([(coef * gap).astype(BF16), *pieces(coef * pick, 2)], axis=0)
        part = contract(left, q_ref[pl.ds(i * CHUNK, CHUNK), :], 1, 0)
        if i == 0:
            acc_ref[...] = part
        else:
            acc_ref[...] += part
    grad = acc_ref[:R, :].T
    weighted = acc_ref[R : R + NM, :] + acc_ref[R + NM :, :]
    model_terms = contract(jnp.concatenate(pieces(weighted, 3), axis=0), proj_ref[...], 1, 0)
    model_grad = model_terms[:NM] + model_terms[NM : 2 * NM] + model_terms[2 * NM :]
    count = out_ref.shape[0]
    for j in range(count):
        for i in range(share // 2):
            at = j * share + 2 * i
            out_ref[j, i] = grad[at : at + 2]
        for i in range(NM // count // 2):
            at = j * (NM // count) + 2 * i
            out_ref[j, share // 2 + i] = model_grad[at : at + 2]


def share_kernel(parts_ref, share_ref, out_ref):
    summed = parts_ref[0]
    for k in range(1, parts_ref.shape[0]):
        summed = summed + parts_ref[k]
    pairs = share_ref.shape[0]
    grad = summed[:pairs]
    share_ref[...] = grad
    square = jnp.sum(grad * grad, axis=0)
    for k in range(out_ref.shape[0]):
        out_ref[k, : summed.shape[0] - pairs] = summed[pairs:]
        out_ref[k, summed.shape[0] - pairs] = square


def pack_kernel(parts_ref, share_ref, loss_ref, out_ref):
    summed = parts_ref[0]
    for k in range(1, parts_ref.shape[0]):
        summed = summed + parts_ref[k]
    pairs = share_ref.shape[0]
    kinds = summed.shape[0] - 1
    model_grad = summed[:kinds]
    square = summed[kinds] + jnp.sum(model_grad * model_grad, axis=0)
    square = jnp.sum(square, axis=0, keepdims=True)
    loss = jnp.sum(loss_ref[...], axis=0, keepdims=True)
    grad = share_ref[...]
    for k in range(out_ref.shape[0]):
        out_ref[k, :pairs] = grad
        out_ref[k, pairs : pairs + kinds] = model_grad
        out_ref[k, pairs + kinds, 0:1] = square
        out_ref[k, pairs + kinds, 1:2] = loss


def final_kernel(share, parts_ref, proj_ref, models_ref, loss_ref):
    count, entries = parts_ref.shape[0], parts_ref.shape[1]
    pairs = share // 2
    kinds = entries - pairs - 1
    sums = parts_ref[0, entries - 1]
    for k in range(1, count):
        sums = sums + parts_ref[k, entries - 1]
    sums = jnp.sum(sums, axis=1, keepdims=True)
    loss_ref[...] = sums[1:2]
    scale = jnp.sqrt(F32(D * R + NM * R)) / (jnp.sqrt(sums[0:1]) + 1e-06)
    scale = jnp.broadcast_to(scale, (2, LANES))
    for k in range(count):
        for i in range(pairs):
            proj_ref[k * share + 2 * i : k * share + 2 * i + 2, :] = scale * parts_ref[k, i]
        for i in range(kinds):
            at = 2 * (k * kinds + i)
            models_ref[at : at + 2, :] = scale * parts_ref[k, pairs + i]


VMEM = pl.BlockSpec(memory_space=pltpu.VMEM)
HBM = pl.BlockSpec(memory_space=pltpu.HBM)


def kernel_call(body, outs, ins, name, limit, cost, in_specs=None, scratch=()):
    flops, moved = cost
    return pl.pallas_call(
        body,
        out_shape=outs,
        in_specs=in_specs or [VMEM] * len(ins),
        out_specs=jax.tree.map(lambda _: VMEM, outs),
        scratch_shapes=scratch,
        compiler_params=pltpu.CompilerParams(vmem_limit_bytes=limit * MIB),
        cost_estimate=pl.CostEstimate(flops=flops, bytes_accessed=moved, transcendentals=0),
        name=name,
    )(*ins)


def shape(*dims, kind=F32):
    return jax.ShapeDtypeStruct(dims, kind)


def body(queries, projection, models, first, second, wins):
    tokens, width = queries.shape
    rows, feats = lax.axis_size(ROWS), lax.axis_size("feat")
    share = width // rows
    kinds = NM // rows // 2
    first, second, wins = (x.reshape(tokens // LANES, LANES) for x in (first, second, wins))
    margins, held = kernel_call(
        margin_kernel,
        (shape(feats, tokens // LANES, LANES), pltpu.VMEM((tokens, width), BF16)),
        (first, second, models, projection, pltpu.with_memory_space_constraint(queries, pltpu.HBM)),
        "margins",
        24,
        (2 * tokens * width * R, tokens * width * 2),
        in_specs=[VMEM] * 4 + [HBM],
        scratch=[pltpu.SemaphoreType.DMA((tokens // CHUNK,))],
    )
    margins = exchange(margins, "feat")
    parts, loss = kernel_call(
        functools.partial(grad_kernel, float(tokens * rows), share),
        (shape(rows, share // 2 + kinds, 2, LANES), shape(tokens // LANES, LANES)),
        (margins, first, second, wins, models, projection, held),
        "grads",
        24,
        (4 * tokens * width * R, tokens * width * 2),
        scratch=[pltpu.VMEM((tokens // LANES, LANES), F32), pltpu.VMEM((R + 2 * NM, width), F32)],
    )
    parts = exchange(parts, ROWS)
    grad_share, parts = kernel_call(
        share_kernel,
        (shape(share // 2, 2, LANES), shape(feats, kinds + 1, 2, LANES)),
        (parts,),
        "shares",
        4,
        (10000, 400000),
    )
    parts = exchange(parts, "feat")
    parts = kernel_call(
        pack_kernel,
        shape(rows, share // 2 + kinds + 1, 2, LANES),
        (parts, grad_share, loss),
        "pack",
        4,
        (10000, 400000),
    )
    parts = exchange(parts, ROWS)
    update_proj, update_models, loss = kernel_call(
        functools.partial(final_kernel, share),
        (shape(width, R), shape(NM, R), shape(1, 1)),
        (parts,),
        "final",
        4,
        (10000, 600000),
    )
    return update_proj, update_models, loss.reshape(())


def solution(mesh):
    split = Mesh(
        mesh.devices.reshape(4, 4, 2, mesh.shape["feat"]), ("rows_0", "rows_1", "rows_2", "feat")
    )
    in_specs = (P(ROWS, "feat"), P("feat", None), P(), P(ROWS), P(ROWS), P(ROWS))
    out_specs = (P("feat", None), P(), P())
    return jax.shard_map(body, mesh=split, in_specs=in_specs, out_specs=out_specs, check_vma=False)
```

```python
import functools

import jax
import jax.numpy as jnp
from jax import lax
from jax.experimental import pallas as pl
from jax.experimental.pallas import tpu as pltpu
from jax.sharding import Mesh
from jax.sharding import PartitionSpec as P

D = 4096
R = 128
NM = 64
LANES = 128
ROWS = ("rows_0", "rows_1", "rows_2")
F32 = jnp.float32
BF16 = jnp.bfloat16
MIB = 1 << 20
BLOCK = 1024
AHEAD = 4
CHUNK = 2048


def exchange(x, axis):
    return lax.all_to_all(x, axis, split_axis=0, concat_axis=0, tiled=True)


def pieces(x, count):
    terms = []
    for _ in range(count):
        term = x.astype(BF16)
        terms.append(term)
        x = x - term.astype(F32)
    return terms


def contract(a, b, dim_a, dim_b):
    return lax.dot_general(a, b, (((dim_a,), (dim_b,)), ((), ())), preferred_element_type=F32)


def model_table(models):
    stacked = jnp.concatenate([term.astype(F32) for term in pieces(models, 3)], axis=0)
    return stacked.T.astype(BF16)


def picks(first_ref, second_ref, start, count):
    labels = lax.broadcasted_iota(jnp.int32, (NM, LANES), 0)
    tiles = []
    for i in range(start // LANES, (start + count) // LANES):
        one = jnp.where(labels == first_ref[i : i + 1, :], 1.0, 0.0)
        two = jnp.where(labels == second_ref[i : i + 1, :], 1.0, 0.0)
        tiles.append(one - two)
    return jnp.concatenate(tiles, axis=1)


def margin_kernel(first_hbm, second_hbm, models_hbm, proj_hbm, q_hbm, out_ref, q_ref, gap_ref, pick_ref, proj_ref, first_ref, second_ref, models_ref, q_sems, sems):
    tokens = q_ref.shape[0]
    small = [(models_hbm, models_ref), (first_hbm, first_ref), (second_hbm, second_ref), (proj_hbm, proj_ref)]
    small = [pltpu.make_async_copy(a, b, sems.at[i]) for i, (a, b) in enumerate(small)]
    for copy in small:
        copy.start()
    blocks = [pl.ds(i * BLOCK, BLOCK) for i in range(tokens // BLOCK)]
    copies = [pltpu.make_async_copy(q_hbm.at[rows, :], q_ref.at[rows, :], q_sems.at[i]) for i, rows in enumerate(blocks)]
    for copy in copies[:AHEAD]:
        copy.start()
    for copy in small[:3]:
        copy.wait()
    table = model_table(models_ref[...])
    for start in range(0, tokens, CHUNK):
        pick = picks(first_ref, second_ref, start, CHUNK).astype(BF16)
        pick_ref[:, start : start + CHUNK] = pick
        gap_ref[:, start : start + CHUNK] = contract(table, jnp.concatenate([pick, pick, pick], axis=0), 1, 0)
    small[3].wait()
    proj = proj_ref[...].astype(F32).T.astype(BF16)
    for start in range(0, tokens, CHUNK):
        for i in range(start // BLOCK, (start + CHUNK) // BLOCK):
            copies[i].wait()
            if i + AHEAD < len(copies):
                copies[i + AHEAD].start()
        routed = contract(proj, q_ref[start : start + CHUNK, :], 1, 1)
        margin = jnp.sum(routed * gap_ref[:, start : start + CHUNK], axis=0, keepdims=True)
        for j in range(CHUNK // LANES):
            row = margin[:, j * LANES : (j + 1) * LANES]
            for k in range(out_ref.shape[0]):
                out_ref[k, start // LANES + j : start // LANES + j + 1, :] = row


def grad_kernel(total, share, margins_ref, wins_ref, gap_ref, pick_ref, proj_ref, q_ref, out_ref, loss_ref, coef_ref, acc_ref):
    tokens = q_ref.shape[0]
    margin = margins_ref[0]
    for k in range(1, margins_ref.shape[0]):
        margin = margin + margins_ref[k]
    sign = 2.0 * wins_ref[...].astype(F32) - 1.0
    wrong = -sign * margin
    loss_ref[...] = jax.nn.softplus(wrong) / total
    coef_ref[...] = -sign * jax.nn.sigmoid(wrong) / total
    for start in range(0, tokens, BLOCK):
        cut = slice(start, start + BLOCK)
        row = start // LANES
        coef = jnp.concatenate([coef_ref[row + j : row + j + 1, :] for j in range(BLOCK // LANES)], axis=1)
        back = (coef * gap_ref[:, cut]).astype(BF16)
        left = jnp.concatenate([back, *pieces(coef * pick_ref[:, cut].astype(F32), 2)], axis=0)
        part = contract(left, q_ref[cut, :], 1, 0)
        if start == 0:
            acc_ref[...] = part
        else:
            acc_ref[...] += part
    grad = acc_ref[:R, :].T
    weighted = acc_ref[R : R + NM, :] + acc_ref[R + NM :, :]
    model_terms = contract(jnp.concatenate(pieces(weighted, 3), axis=0), proj_ref[...], 1, 0)
    model_grad = model_terms[:NM] + model_terms[NM : 2 * NM] + model_terms[2 * NM :]
    count = out_ref.shape[0]
    for j in range(count):
        for i in range(share // 2):
            at = j * share + 2 * i
            out_ref[j, i] = grad[at : at + 2]
        for i in range(NM // count // 2):
            at = j * (NM // count) + 2 * i
            out_ref[j, share // 2 + i] = model_grad[at : at + 2]


def share_kernel(parts_ref, share_ref, out_ref):
    summed = parts_ref[0]
    for k in range(1, parts_ref.shape[0]):
        summed = summed + parts_ref[k]
    pairs = share_ref.shape[0]
    grad = summed[:pairs]
    share_ref[...] = grad
    square = jnp.sum(grad * grad, axis=0)
    for k in range(out_ref.shape[0]):
        out_ref[k, : summed.shape[0] - pairs] = summed[pairs:]
        out_ref[k, summed.shape[0] - pairs] = square


def pack_kernel(parts_ref, share_ref, loss_ref, out_ref):
    summed = parts_ref[0]
    for k in range(1, parts_ref.shape[0]):
        summed = summed + parts_ref[k]
    pairs = share_ref.shape[0]
    kinds = summed.shape[0] - 1
    model_grad = summed[:kinds]
    square = summed[kinds] + jnp.sum(model_grad * model_grad, axis=0)
    square = jnp.sum(square, axis=0, keepdims=True)
    loss = jnp.sum(loss_ref[...], axis=0, keepdims=True)
    grad = share_ref[...]
    for k in range(out_ref.shape[0]):
        out_ref[k, :pairs] = grad
        out_ref[k, pairs : pairs + kinds] = model_grad
        out_ref[k, pairs + kinds, 0:1] = square
        out_ref[k, pairs + kinds, 1:2] = loss


def final_kernel(share, parts_ref, proj_ref, models_ref, loss_ref):
    count, entries = parts_ref.shape[0], parts_ref.shape[1]
    pairs = share // 2
    kinds = entries - pairs - 1
    sums = parts_ref[0, entries - 1]
    for k in range(1, count):
        sums = sums + parts_ref[k, entries - 1]
    sums = jnp.sum(sums, axis=1, keepdims=True)
    loss_ref[...] = sums[1:2]
    scale = jnp.sqrt(F32(D * R + NM * R)) / (jnp.sqrt(sums[0:1]) + 1e-06)
    scale = jnp.broadcast_to(scale, (2, LANES))
    for k in range(count):
        for i in range(pairs):
            proj_ref[k * share + 2 * i : k * share + 2 * i + 2, :] = scale * parts_ref[k, i]
        for i in range(kinds):
            at = 2 * (k * kinds + i)
            models_ref[at : at + 2, :] = scale * parts_ref[k, pairs + i]


VMEM = pl.BlockSpec(memory_space=pltpu.VMEM)
HBM = pl.BlockSpec(memory_space=pltpu.HBM)


def kernel_call(body, outs, ins, name, limit, cost, in_specs=None, scratch=()):
    flops, moved = cost
    return pl.pallas_call(
        body,
        out_shape=outs,
        in_specs=in_specs or [VMEM] * len(ins),
        out_specs=jax.tree.map(lambda _: VMEM, outs),
        scratch_shapes=scratch,
        compiler_params=pltpu.CompilerParams(vmem_limit_bytes=limit * MIB),
        cost_estimate=pl.CostEstimate(flops=flops, bytes_accessed=moved, transcendentals=0),
        name=name,
    )(*ins)


def shape(*dims, kind=F32):
    return jax.ShapeDtypeStruct(dims, kind)


def body(queries, projection, models, first, second, wins):
    tokens, width = queries.shape
    rows, feats = lax.axis_size(ROWS), lax.axis_size("feat")
    share = width // rows
    kinds = NM // rows // 2
    first, second, wins = (x.reshape(tokens // LANES, LANES) for x in (first, second, wins))
    sources = (first, second, models, projection, queries)
    margins, held, gap, pick, proj = kernel_call(
        margin_kernel,
        (
            shape(feats, tokens // LANES, LANES),
            pltpu.VMEM((tokens, width), BF16),
            pltpu.VMEM((R, tokens), F32),
            pltpu.VMEM((NM, tokens), BF16),
            pltpu.VMEM(projection.shape, BF16),
        ),
        [pltpu.with_memory_space_constraint(x, pltpu.HBM) for x in sources],
        "margins",
        24,
        (2 * tokens * width * R, tokens * width * 2),
        in_specs=[HBM] * len(sources),
        scratch=[
            pltpu.VMEM(first.shape, jnp.int32),
            pltpu.VMEM(first.shape, jnp.int32),
            pltpu.VMEM(models.shape, F32),
            pltpu.SemaphoreType.DMA((tokens // BLOCK,)),
            pltpu.SemaphoreType.DMA((4,)),
        ],
    )
    margins = exchange(margins, "feat")
    parts, loss = kernel_call(
        functools.partial(grad_kernel, float(tokens * rows), share),
        (shape(rows, share // 2 + kinds, 2, LANES), shape(tokens // LANES, LANES)),
        (margins, wins, gap, pick, proj, held),
        "grads",
        24,
        (4 * tokens * width * R, tokens * width * 2),
        scratch=[pltpu.VMEM((tokens // LANES, LANES), F32), pltpu.VMEM((R + 2 * NM, width), F32)],
    )
    parts = exchange(parts, ROWS)
    grad_share, parts = kernel_call(
        share_kernel,
        (shape(share // 2, 2, LANES), shape(feats, kinds + 1, 2, LANES)),
        (parts,),
        "shares",
        4,
        (10000, 400000),
    )
    parts = exchange(parts, "feat")
    parts = kernel_call(
        pack_kernel,
        shape(rows, share // 2 + kinds + 1, 2, LANES),
        (parts, grad_share, loss),
        "pack",
        4,
        (10000, 400000),
    )
    parts = exchange(parts, ROWS)
    update_proj, update_models, loss = kernel_call(
        functools.partial(final_kernel, share),
        (shape(width, R), shape(NM, R), shape(1, 1)),
        (parts,),
        "final",
        4,
        (10000, 600000),
    )
    return update_proj, update_models, loss.reshape(())


def solution(mesh):
    split = Mesh(
        mesh.devices.reshape(4, 4, 2, mesh.shape["feat"]), ("rows_0", "rows_1", "rows_2", "feat")
    )
    in_specs = (P(ROWS, "feat"), P("feat", None), P(), P(ROWS), P(ROWS), P(ROWS))
    out_specs = (P("feat", None), P(), P())
    return jax.shard_map(body, mesh=split, in_specs=in_specs, out_specs=out_specs, check_vma=False)
```

```python
import functools

import jax
import jax.numpy as jnp
from jax import lax
from jax.experimental import pallas as pl
from jax.experimental.pallas import tpu as pltpu
from jax.sharding import Mesh
from jax.sharding import PartitionSpec as P

D = 4096
R = 128
NM = 64
LANES = 128
ROWS = ("rows_0", "rows_1", "rows_2")
F32 = jnp.float32
BF16 = jnp.bfloat16
MIB = 1 << 20
BLOCK = 1024
AHEAD = 2
CHUNK = 2048


def exchange(x, axis):
    return lax.all_to_all(x, axis, split_axis=0, concat_axis=0, tiled=True)


def pieces(x, count):
    terms = []
    for _ in range(count):
        term = x.astype(BF16)
        terms.append(term)
        x = x - term.astype(F32)
    return terms


def contract(a, b, dim_a, dim_b):
    return lax.dot_general(a, b, (((dim_a,), (dim_b,)), ((), ())), preferred_element_type=F32)


def model_table(models):
    stacked = jnp.concatenate([term.astype(F32) for term in pieces(models, 3)], axis=0)
    return stacked.T.astype(BF16)


def picks(first_ref, second_ref, start, count):
    labels = lax.broadcasted_iota(jnp.int32, (NM, LANES), 0)
    tiles = []
    for i in range(start // LANES, (start + count) // LANES):
        one = jnp.where(labels == first_ref[i : i + 1, :], 1.0, 0.0)
        two = jnp.where(labels == second_ref[i : i + 1, :], 1.0, 0.0)
        tiles.append(one - two)
    return jnp.concatenate(tiles, axis=1)


def margin_kernel(first_hbm, second_hbm, models_hbm, proj_hbm, q_hbm, out_ref, q_ref, gap_ref, pick_ref, proj_ref, first_ref, second_ref, models_ref, q_sems, sems):
    tokens = q_ref.shape[0]
    small = [(models_hbm, models_ref), (first_hbm, first_ref), (second_hbm, second_ref), (proj_hbm, proj_ref)]
    small = [pltpu.make_async_copy(a, b, sems.at[i]) for i, (a, b) in enumerate(small)]
    for copy in small:
        copy.start()
    blocks = [pl.ds(i * BLOCK, BLOCK) for i in range(tokens // BLOCK)]
    copies = [pltpu.make_async_copy(q_hbm.at[rows, :], q_ref.at[rows, :], q_sems.at[i]) for i, rows in enumerate(blocks)]
    for copy in copies[:AHEAD]:
        copy.start()
    for copy in small[:3]:
        copy.wait()
    table = model_table(models_ref[...])
    started = AHEAD
    for start in range(0, tokens, BLOCK):
        cut = slice(start, start + BLOCK)
        pick = picks(first_ref, second_ref, start, BLOCK).astype(BF16)
        pick_ref[:, cut] = pick
        gap_ref[:, cut] = contract(table, jnp.concatenate([pick, pick, pick], axis=0), 1, 0)
        if start > 0 and started < len(copies):
            copies[started].start()
            started += 1
    small[3].wait()
    proj = proj_ref[...].astype(F32).T.astype(BF16)
    for start in range(0, tokens, CHUNK):
        for i in range(start // BLOCK, (start + CHUNK) // BLOCK):
            copies[i].wait()
        routed = contract(proj, q_ref[start : start + CHUNK, :], 1, 1)
        margin = jnp.sum(routed * gap_ref[:, start : start + CHUNK], axis=0, keepdims=True)
        for j in range(CHUNK // LANES):
            row = margin[:, j * LANES : (j + 1) * LANES]
            for k in range(out_ref.shape[0]):
                out_ref[k, start // LANES + j : start // LANES + j + 1, :] = row


def grad_kernel(total, share, margins_ref, wins_ref, gap_ref, pick_ref, proj_ref, q_ref, out_ref, loss_ref, coef_ref, acc_ref):
    tokens = q_ref.shape[0]
    margin = margins_ref[0]
    for k in range(1, margins_ref.shape[0]):
        margin = margin + margins_ref[k]
    sign = 2.0 * wins_ref[...].astype(F32) - 1.0
    wrong = -sign * margin
    loss_ref[...] = jax.nn.softplus(wrong) / total
    coef_ref[...] = -sign * jax.nn.sigmoid(wrong) / total
    for start in range(0, tokens, BLOCK):
        cut = slice(start, start + BLOCK)
        row = start // LANES
        coef = jnp.concatenate([coef_ref[row + j : row + j + 1, :] for j in range(BLOCK // LANES)], axis=1)
        back = (coef * gap_ref[:, cut]).astype(BF16)
        left = jnp.concatenate([back, *pieces(coef * pick_ref[:, cut].astype(F32), 2)], axis=0)
        part = contract(left, q_ref[cut, :], 1, 0)
        if start == 0:
            acc_ref[...] = part
        else:
            acc_ref[...] += part
    grad = acc_ref[:R, :].T
    weighted = acc_ref[R : R + NM, :] + acc_ref[R + NM :, :]
    model_terms = contract(jnp.concatenate(pieces(weighted, 3), axis=0), proj_ref[...], 1, 0)
    model_grad = model_terms[:NM] + model_terms[NM : 2 * NM] + model_terms[2 * NM :]
    count = out_ref.shape[0]
    for j in range(count):
        for i in range(share // 2):
            at = j * share + 2 * i
            out_ref[j, i] = grad[at : at + 2]
        for i in range(NM // count // 2):
            at = j * (NM // count) + 2 * i
            out_ref[j, share // 2 + i] = model_grad[at : at + 2]


def share_kernel(parts_ref, share_ref, out_ref):
    summed = parts_ref[0]
    for k in range(1, parts_ref.shape[0]):
        summed = summed + parts_ref[k]
    pairs = share_ref.shape[0]
    grad = summed[:pairs]
    share_ref[...] = grad
    square = jnp.sum(grad * grad, axis=0)
    for k in range(out_ref.shape[0]):
        out_ref[k, : summed.shape[0] - pairs] = summed[pairs:]
        out_ref[k, summed.shape[0] - pairs] = square


def pack_kernel(parts_ref, share_ref, loss_ref, out_ref):
    summed = parts_ref[0]
    for k in range(1, parts_ref.shape[0]):
        summed = summed + parts_ref[k]
    pairs = share_ref.shape[0]
    kinds = summed.shape[0] - 1
    model_grad = summed[:kinds]
    square = summed[kinds] + jnp.sum(model_grad * model_grad, axis=0)
    square = jnp.sum(square, axis=0, keepdims=True)
    loss = jnp.sum(loss_ref[...], axis=0, keepdims=True)
    grad = share_ref[...]
    for k in range(out_ref.shape[0]):
        out_ref[k, :pairs] = grad
        out_ref[k, pairs : pairs + kinds] = model_grad
        out_ref[k, pairs + kinds, 0:1] = square
        out_ref[k, pairs + kinds, 1:2] = loss


def final_kernel(share, parts_ref, proj_ref, models_ref, loss_ref):
    count, entries = parts_ref.shape[0], parts_ref.shape[1]
    pairs = share // 2
    kinds = entries - pairs - 1
    sums = parts_ref[0, entries - 1]
    for k in range(1, count):
        sums = sums + parts_ref[k, entries - 1]
    sums = jnp.sum(sums, axis=1, keepdims=True)
    loss_ref[...] = sums[1:2]
    scale = jnp.sqrt(F32(D * R + NM * R)) / (jnp.sqrt(sums[0:1]) + 1e-06)
    scale = jnp.broadcast_to(scale, (2, LANES))
    for k in range(count):
        for i in range(pairs):
            proj_ref[k * share + 2 * i : k * share + 2 * i + 2, :] = scale * parts_ref[k, i]
        for i in range(kinds):
            at = 2 * (k * kinds + i)
            models_ref[at : at + 2, :] = scale * parts_ref[k, pairs + i]


VMEM = pl.BlockSpec(memory_space=pltpu.VMEM)
HBM = pl.BlockSpec(memory_space=pltpu.HBM)


def kernel_call(body, outs, ins, name, limit, cost, in_specs=None, scratch=()):
    flops, moved = cost
    return pl.pallas_call(
        body,
        out_shape=outs,
        in_specs=in_specs or [VMEM] * len(ins),
        out_specs=jax.tree.map(lambda _: VMEM, outs),
        scratch_shapes=scratch,
        compiler_params=pltpu.CompilerParams(vmem_limit_bytes=limit * MIB),
        cost_estimate=pl.CostEstimate(flops=flops, bytes_accessed=moved, transcendentals=0),
        name=name,
    )(*ins)


def shape(*dims, kind=F32):
    return jax.ShapeDtypeStruct(dims, kind)


def body(queries, projection, models, first, second, wins):
    tokens, width = queries.shape
    rows, feats = lax.axis_size(ROWS), lax.axis_size("feat")
    share = width // rows
    kinds = NM // rows // 2
    first, second, wins = (x.reshape(tokens // LANES, LANES) for x in (first, second, wins))
    sources = (first, second, models, projection, queries)
    margins, held, gap, pick, proj = kernel_call(
        margin_kernel,
        (
            shape(feats, tokens // LANES, LANES),
            pltpu.VMEM((tokens, width), BF16),
            pltpu.VMEM((R, tokens), F32),
            pltpu.VMEM((NM, tokens), BF16),
            pltpu.VMEM(projection.shape, BF16),
        ),
        [pltpu.with_memory_space_constraint(x, pltpu.HBM) for x in sources],
        "margins",
        24,
        (2 * tokens * width * R, tokens * width * 2),
        in_specs=[HBM] * len(sources),
        scratch=[
            pltpu.VMEM(first.shape, jnp.int32),
            pltpu.VMEM(first.shape, jnp.int32),
            pltpu.VMEM(models.shape, F32),
            pltpu.SemaphoreType.DMA((tokens // BLOCK,)),
            pltpu.SemaphoreType.DMA((4,)),
        ],
    )
    margins = exchange(margins, "feat")
    parts, loss = kernel_call(
        functools.partial(grad_kernel, float(tokens * rows), share),
        (shape(rows, share // 2 + kinds, 2, LANES), shape(tokens // LANES, LANES)),
        (margins, wins, gap, pick, proj, held),
        "grads",
        24,
        (4 * tokens * width * R, tokens * width * 2),
        scratch=[pltpu.VMEM((tokens // LANES, LANES), F32), pltpu.VMEM((R + 2 * NM, width), F32)],
    )
    parts = exchange(parts, ROWS)
    grad_share, parts = kernel_call(
        share_kernel,
        (shape(share // 2, 2, LANES), shape(feats, kinds + 1, 2, LANES)),
        (parts,),
        "shares",
        4,
        (10000, 400000),
    )
    parts = exchange(parts, "feat")
    parts = kernel_call(
        pack_kernel,
        shape(rows, share // 2 + kinds + 1, 2, LANES),
        (parts, grad_share, loss),
        "pack",
        4,
        (10000, 400000),
    )
    parts = exchange(parts, ROWS)
    update_proj, update_models, loss = kernel_call(
        functools.partial(final_kernel, share),
        (shape(width, R), shape(NM, R), shape(1, 1)),
        (parts,),
        "final",
        4,
        (10000, 600000),
    )
    return update_proj, update_models, loss.reshape(())


def solution(mesh):
    split = Mesh(
        mesh.devices.reshape(4, 4, 2, mesh.shape["feat"]), ("rows_0", "rows_1", "rows_2", "feat")
    )
    in_specs = (P(ROWS, "feat"), P("feat", None), P(), P(ROWS), P(ROWS), P(ROWS))
    out_specs = (P("feat", None), P(), P())
    return jax.shard_map(body, mesh=split, in_specs=in_specs, out_specs=out_specs, check_vma=False)
```

```python
import functools

import jax
import jax.numpy as jnp
from jax import lax
from jax.experimental import pallas as pl
from jax.experimental.pallas import tpu as pltpu
from jax.sharding import Mesh
from jax.sharding import PartitionSpec as P

D = 4096
R = 128
NM = 64
LANES = 128
CORE = "rows_2"
CHIPS = ("rows_0", "rows_1")
ROWS = (*CHIPS, CORE)
F32 = jnp.float32
BF16 = jnp.bfloat16
MIB = 1 << 20
BLOCK = 1024
AHEAD = 2
CHUNK = 2048


def exchange(x, axis):
    return lax.all_to_all(x, axis, split_axis=0, concat_axis=0, tiled=True)


def swap(x):
    return lax.ppermute(x, CORE, [(0, 1), (1, 0)])


def pieces(x, count):
    terms = []
    for _ in range(count):
        term = x.astype(BF16)
        terms.append(term)
        x = x - term.astype(F32)
    return terms


def contract(a, b, dim_a, dim_b):
    return lax.dot_general(a, b, (((dim_a,), (dim_b,)), ((), ())), preferred_element_type=F32)


def model_table(models):
    stacked = jnp.concatenate([term.astype(F32) for term in pieces(models, 3)], axis=0)
    return stacked.T.astype(BF16)


def picks(first_ref, second_ref, start, count):
    labels = lax.broadcasted_iota(jnp.int32, (NM, LANES), 0)
    tiles = []
    for i in range(start // LANES, (start + count) // LANES):
        one = jnp.where(labels == first_ref[i : i + 1, :], 1.0, 0.0)
        two = jnp.where(labels == second_ref[i : i + 1, :], 1.0, 0.0)
        tiles.append(one - two)
    return jnp.concatenate(tiles, axis=1)


def halve(x, flip):
    half = x.shape[0] // 2
    return jnp.where(flip, x[half:], x[:half]), jnp.where(flip, x[:half], x[half:])


def margin_kernel(first_hbm, second_hbm, models_hbm, proj_hbm, q_hbm, out_ref, q_ref, gap_ref, pick_ref, proj_ref, first_ref, second_ref, models_ref, q_sems, sems):
    tokens = q_ref.shape[0]
    small = [(models_hbm, models_ref), (first_hbm, first_ref), (second_hbm, second_ref), (proj_hbm, proj_ref)]
    small = [pltpu.make_async_copy(a, b, sems.at[i]) for i, (a, b) in enumerate(small)]
    for copy in small:
        copy.start()
    blocks = [pl.ds(i * BLOCK, BLOCK) for i in range(tokens // BLOCK)]
    copies = [pltpu.make_async_copy(q_hbm.at[rows, :], q_ref.at[rows, :], q_sems.at[i]) for i, rows in enumerate(blocks)]
    for copy in copies[:AHEAD]:
        copy.start()
    for copy in small[:3]:
        copy.wait()
    table = model_table(models_ref[...])
    started = AHEAD
    for start in range(0, tokens, BLOCK):
        cut = slice(start, start + BLOCK)
        pick = picks(first_ref, second_ref, start, BLOCK).astype(BF16)
        pick_ref[:, cut] = pick
        gap_ref[:, cut] = contract(table, jnp.concatenate([pick, pick, pick], axis=0), 1, 0)
        if start > 0 and started < len(copies):
            copies[started].start()
            started += 1
    small[3].wait()
    proj = proj_ref[...].astype(F32).T.astype(BF16)
    for start in range(0, tokens, CHUNK):
        for i in range(start // BLOCK, (start + CHUNK) // BLOCK):
            copies[i].wait()
        routed = contract(proj, q_ref[start : start + CHUNK, :], 1, 1)
        margin = jnp.sum(routed * gap_ref[:, start : start + CHUNK], axis=0, keepdims=True)
        for j in range(CHUNK // LANES):
            row = margin[:, j * LANES : (j + 1) * LANES]
            for k in range(out_ref.shape[0]):
                out_ref[k, start // LANES + j : start // LANES + j + 1, :] = row


def grad_kernel(total, share, margins_ref, wins_ref, gap_ref, pick_ref, proj_ref, q_ref, own_ref, other_ref, loss_ref, coef_ref, acc_ref):
    tokens = q_ref.shape[0]
    margin = margins_ref[0]
    for k in range(1, margins_ref.shape[0]):
        margin = margin + margins_ref[k]
    sign = 2.0 * wins_ref[...].astype(F32) - 1.0
    wrong = -sign * margin
    loss_ref[...] = jax.nn.softplus(wrong) / total
    coef_ref[...] = -sign * jax.nn.sigmoid(wrong) / total
    for start in range(0, tokens, BLOCK):
        cut = slice(start, start + BLOCK)
        row = start // LANES
        coef = jnp.concatenate([coef_ref[row + j : row + j + 1, :] for j in range(BLOCK // LANES)], axis=1)
        back = (coef * gap_ref[:, cut]).astype(BF16)
        left = jnp.concatenate([back, *pieces(coef * pick_ref[:, cut].astype(F32), 2)], axis=0)
        part = contract(left, q_ref[cut, :], 1, 0)
        if start == 0:
            acc_ref[...] = part
        else:
            acc_ref[...] += part
    grad = acc_ref[:R, :].T
    weighted = acc_ref[R : R + NM, :] + acc_ref[R + NM :, :]
    model_terms = contract(jnp.concatenate(pieces(weighted, 3), axis=0), proj_ref[...], 1, 0)
    model_grad = model_terms[:NM] + model_terms[NM : 2 * NM] + model_terms[2 * NM :]
    flip = lax.axis_index(CORE) == 1
    halves = [halve(x, flip) for x in (grad, model_grad)]
    count = own_ref.shape[0]
    for ref, grad, model_grad in zip((own_ref, other_ref), *halves):
        for j in range(count):
            for i in range(share // 2):
                at = j * share + 2 * i
                ref[j, i] = grad[at : at + 2]
            for i in range(NM // 2 // count // 2):
                at = j * (NM // 2 // count) + 2 * i
                ref[j, share // 2 + i] = model_grad[at : at + 2]


def share_kernel(parts_ref, share_ref, out_ref):
    summed = parts_ref[0]
    for k in range(1, parts_ref.shape[0]):
        summed = summed + parts_ref[k]
    pairs = share_ref.shape[0]
    grad = summed[:pairs]
    share_ref[...] = grad
    square = jnp.sum(grad * grad, axis=0)
    for k in range(out_ref.shape[0]):
        out_ref[k, : summed.shape[0] - pairs] = summed[pairs:]
        out_ref[k, summed.shape[0] - pairs] = square


def pack_kernel(parts_ref, share_ref, loss_ref, out_ref):
    summed = parts_ref[0]
    for k in range(1, parts_ref.shape[0]):
        summed = summed + parts_ref[k]
    pairs = share_ref.shape[0]
    kinds = summed.shape[0] - 1
    model_grad = summed[:kinds]
    square = summed[kinds] + jnp.sum(model_grad * model_grad, axis=0)
    square = jnp.sum(square, axis=0, keepdims=True)
    loss = jnp.sum(loss_ref[...], axis=0, keepdims=True)
    grad = share_ref[...]
    for k in range(out_ref.shape[0]):
        out_ref[k, :pairs] = grad
        out_ref[k, pairs : pairs + kinds] = model_grad
        out_ref[k, pairs + kinds, 0:1] = square
        out_ref[k, pairs + kinds, 1:2] = loss


def final_kernel(share, own_ref, other_ref, proj_ref, models_ref, loss_ref):
    count, entries = own_ref.shape[0], own_ref.shape[1]
    pairs = share // 2
    kinds = entries - pairs - 1
    sums = own_ref[0, entries - 1] + other_ref[0, entries - 1]
    for k in range(1, count):
        sums = sums + (own_ref[k, entries - 1] + other_ref[k, entries - 1])
    sums = jnp.sum(sums, axis=1, keepdims=True)
    loss_ref[...] = sums[1:2]
    scale = jnp.sqrt(F32(D * R + NM * R)) / (jnp.sqrt(sums[0:1]) + 1e-06)
    scale = jnp.broadcast_to(scale, (2, LANES))
    flip = lax.axis_index(CORE) == 1
    for k in range(count):
        for i in range(pairs + kinds):
            own, other = scale * own_ref[k, i], scale * other_ref[k, i]
            for c, rows in enumerate((jnp.where(flip, other, own), jnp.where(flip, own, other))):
                if i < pairs:
                    at = (c * count + k) * share + 2 * i
                    proj_ref[at : at + 2, :] = rows
                else:
                    at = 2 * ((c * count + k) * kinds + i - pairs)
                    models_ref[at : at + 2, :] = rows


VMEM = pl.BlockSpec(memory_space=pltpu.VMEM)
HBM = pl.BlockSpec(memory_space=pltpu.HBM)


def kernel_call(body, outs, ins, name, limit, cost, in_specs=None, scratch=()):
    flops, moved = cost
    return pl.pallas_call(
        body,
        out_shape=outs,
        in_specs=in_specs or [VMEM] * len(ins),
        out_specs=jax.tree.map(lambda _: VMEM, outs),
        scratch_shapes=scratch,
        compiler_params=pltpu.CompilerParams(vmem_limit_bytes=limit * MIB),
        cost_estimate=pl.CostEstimate(flops=flops, bytes_accessed=moved, transcendentals=0),
        name=name,
    )(*ins)


def shape(*dims, kind=F32):
    return jax.ShapeDtypeStruct(dims, kind)


def body(queries, projection, models, first, second, wins):
    tokens, width = queries.shape
    rows, chips, feats = lax.axis_size(ROWS), lax.axis_size(CHIPS), lax.axis_size("feat")
    share = width // rows
    kinds = NM // rows // 2
    first, second, wins = (x.reshape(tokens // LANES, LANES) for x in (first, second, wins))
    sources = (first, second, models, projection, queries)
    margins, held, gap, pick, proj = kernel_call(
        margin_kernel,
        (
            shape(feats, tokens // LANES, LANES),
            pltpu.VMEM((tokens, width), BF16),
            pltpu.VMEM((R, tokens), F32),
            pltpu.VMEM((NM, tokens), BF16),
            pltpu.VMEM(projection.shape, BF16),
        ),
        [pltpu.with_memory_space_constraint(x, pltpu.HBM) for x in sources],
        "margins",
        24,
        (2 * tokens * width * R, tokens * width * 2),
        in_specs=[HBM] * len(sources),
        scratch=[
            pltpu.VMEM(first.shape, jnp.int32),
            pltpu.VMEM(first.shape, jnp.int32),
            pltpu.VMEM(models.shape, F32),
            pltpu.SemaphoreType.DMA((tokens // BLOCK,)),
            pltpu.SemaphoreType.DMA((4,)),
        ],
    )
    margins = exchange(margins, "feat")
    packed = shape(chips, share // 2 + kinds, 2, LANES)
    own, other, loss = kernel_call(
        functools.partial(grad_kernel, float(tokens * rows), share),
        (packed, packed, shape(tokens // LANES, LANES)),
        (margins, wins, gap, pick, proj, held),
        "grads",
        24,
        (4 * tokens * width * R, tokens * width * 2),
        scratch=[pltpu.VMEM((tokens // LANES, LANES), F32), pltpu.VMEM((R + 2 * NM, width), F32)],
    )
    parts = exchange(own + swap(other), CHIPS)
    grad_share, parts = kernel_call(
        share_kernel,
        (shape(share // 2, 2, LANES), shape(feats, kinds + 1, 2, LANES)),
        (parts,),
        "shares",
        4,
        (10000, 400000),
    )
    parts = exchange(parts, "feat")
    parts = kernel_call(
        pack_kernel,
        shape(chips, share // 2 + kinds + 1, 2, LANES),
        (parts, grad_share, loss),
        "pack",
        4,
        (10000, 400000),
    )
    parts = exchange(parts, CHIPS)
    update_proj, update_models, loss = kernel_call(
        functools.partial(final_kernel, share),
        (shape(width, R), shape(NM, R), shape(1, 1)),
        (parts, swap(parts)),
        "final",
        4,
        (10000, 600000),
    )
    return update_proj, update_models, loss.reshape(())


def solution(mesh):
    split = Mesh(
        mesh.devices.reshape(4, 4, 2, mesh.shape["feat"]), ("rows_0", "rows_1", "rows_2", "feat")
    )
    in_specs = (P(ROWS, "feat"), P("feat", None), P(), P(ROWS), P(ROWS), P(ROWS))
    out_specs = (P("feat", None), P(), P())
    return jax.shard_map(body, mesh=split, in_specs=in_specs, out_specs=out_specs, check_vma=False)
```

```python
import functools

import jax
import jax.numpy as jnp
from jax import lax
from jax.experimental import pallas as pl
from jax.experimental.pallas import tpu as pltpu
from jax.sharding import Mesh
from jax.sharding import PartitionSpec as P


D = 4096
R = 128
NM = 64
LANES = 128
CORE = "rows_2"
CHIPS = ("rows_0", "rows_1")
ROWS = (*CHIPS, CORE)
F32 = jnp.float32
BF16 = jnp.bfloat16
MIB = 1 << 20
BLOCK = 1024
AHEAD = 2
CHUNK = 2048


def exchange(x, axis):
    return lax.all_to_all(x, axis, split_axis=0, concat_axis=0, tiled=True)


def swap(x):
    return lax.ppermute(x, CORE, [(0, 1), (1, 0)])


def pieces(x, count):
    terms = []
    for _ in range(count):
        term = x.astype(BF16)
        terms.append(term)
        x = x - term.astype(F32)
    return terms


def contract(a, b, dim_a, dim_b):
    return lax.dot_general(a, b, (((dim_a,), (dim_b,)), ((), ())), preferred_element_type=F32)


def model_table(models):
    stacked = jnp.concatenate([term.astype(F32) for term in pieces(models, 3)], axis=0)
    return stacked.T.astype(BF16)


def picks(first_ref, second_ref, start, count):
    labels = lax.broadcasted_iota(jnp.int32, (NM, LANES), 0)
    tiles = []
    for i in range(start // LANES, (start + count) // LANES):
        one = jnp.where(labels == first_ref[i : i + 1, :], 1.0, 0.0)
        two = jnp.where(labels == second_ref[i : i + 1, :], 1.0, 0.0)
        tiles.append(one - two)
    return jnp.concatenate(tiles, axis=1)


def margin_kernel(first_hbm, second_hbm, models_hbm, proj_hbm, q_hbm, out_ref, q_ref, gap_ref, pick_ref, proj_ref, first_ref, second_ref, models_ref, q_sems, sems):
    tokens = q_ref.shape[0]
    small = [(models_hbm, models_ref), (first_hbm, first_ref), (second_hbm, second_ref), (proj_hbm, proj_ref)]
    small = [pltpu.make_async_copy(a, b, sems.at[i]) for i, (a, b) in enumerate(small)]
    for copy in small:
        copy.start()
    blocks = [pl.ds(i * BLOCK, BLOCK) for i in range(tokens // BLOCK)]
    copies = [pltpu.make_async_copy(q_hbm.at[rows, :], q_ref.at[rows, :], q_sems.at[i]) for i, rows in enumerate(blocks)]
    for copy in copies[:AHEAD]:
        copy.start()
    for copy in small[:3]:
        copy.wait()
    table = model_table(models_ref[...])
    started = AHEAD
    for start in range(0, tokens, BLOCK):
        cut = slice(start, start + BLOCK)
        pick = picks(first_ref, second_ref, start, BLOCK).astype(BF16)
        pick_ref[:, cut] = pick
        gap_ref[:, cut] = contract(table, jnp.concatenate([pick, pick, pick], axis=0), 1, 0)
        if start > 0 and started < len(copies):
            copies[started].start()
            started += 1
    small[3].wait()
    proj = proj_ref[...].astype(F32).T.astype(BF16)
    for start in range(0, tokens, CHUNK):
        for i in range(start // BLOCK, (start + CHUNK) // BLOCK):
            copies[i].wait()
        routed = contract(proj, q_ref[start : start + CHUNK, :], 1, 1)
        margin = jnp.sum(routed * gap_ref[:, start : start + CHUNK], axis=0, keepdims=True)
        for j in range(CHUNK // LANES):
            row = margin[:, j * LANES : (j + 1) * LANES]
            for k in range(out_ref.shape[0]):
                out_ref[k, start // LANES + j : start // LANES + j + 1, :] = row


def put_pairs(ref, at, rows):
    count = ref.shape[0]
    pairs = rows.shape[0] // count // 2
    for j in range(count):
        for i in range(pairs):
            row = 2 * (j * pairs + i)
            ref[j, at + i] = rows[row : row + 2]


def columns(half, width):
    return pl.ds(pl.multiple_of(half * width, width), width)


def other_kernel(total, margins_ref, wins_ref, gap_ref, pick_ref, q_ref, out_ref, loss_ref, left_ref, weighted_ref, coef_ref, acc_ref):
    tokens = q_ref.shape[0]
    width = acc_ref.shape[1]
    margin = margins_ref[0]
    for k in range(1, margins_ref.shape[0]):
        margin = margin + margins_ref[k]
    sign = 2.0 * wins_ref[...].astype(F32) - 1.0
    wrong = -sign * margin
    loss_ref[...] = jax.nn.softplus(wrong) / total
    coef_ref[...] = -sign * jax.nn.sigmoid(wrong) / total
    other = columns(1 - lax.axis_index(CORE), width)
    for start in range(0, tokens, BLOCK):
        cut = slice(start, start + BLOCK)
        row = start // LANES
        coef = jnp.concatenate([coef_ref[row + j : row + j + 1, :] for j in range(BLOCK // LANES)], axis=1)
        back = (coef * gap_ref[:, cut]).astype(BF16)
        left = jnp.concatenate([back, *pieces(coef * pick_ref[:, cut].astype(F32), 2)], axis=0)
        left_ref[:, cut] = left
        part = contract(left, q_ref[cut, other], 1, 0)
        if start == 0:
            acc_ref[...] = part
        else:
            acc_ref[...] += part
    put_pairs(out_ref, 0, acc_ref[:R, :].T)
    weighted_ref[...] = acc_ref[R : R + NM, :] + acc_ref[R + NM :, :]


def own_kernel(left_ref, weighted_ref, proj_ref, q_ref, out_ref, models_ref):
    width = weighted_ref.shape[1]
    core = lax.axis_index(CORE)
    acc = contract(left_ref[...], q_ref[:, columns(core, width)], 1, 0)
    put_pairs(out_ref, 0, acc[:R].T)
    model_grad = jnp.zeros((NM, R), F32)
    for half, weighted in ((core, acc[R : R + NM] + acc[R + NM :]), (1 - core, weighted_ref[...])):
        terms = contract(jnp.concatenate(pieces(weighted, 3), axis=0), proj_ref[columns(half, width), :], 1, 0)
        model_grad = model_grad + (terms[:NM] + terms[NM : 2 * NM] + terms[2 * NM :])
    put_pairs(models_ref, 0, model_grad)


def join_kernel(own_ref, other_ref, models_ref, out_ref):
    pairs = own_ref.shape[1]
    out_ref[:, :pairs] = own_ref[...] + other_ref[...]
    out_ref[:, pairs:] = models_ref[...]


def share_kernel(feats, parts_ref, loss_ref, share_ref, out_ref):
    summed = parts_ref[0]
    for k in range(1, parts_ref.shape[0]):
        summed = summed + parts_ref[k]
    pairs = share_ref.shape[0]
    kinds = summed.shape[0] - pairs
    grad = summed[:pairs]
    share_ref[...] = grad
    square = jnp.sum(jnp.sum(grad * grad, axis=0), axis=0, keepdims=True)
    loss = jnp.sum(loss_ref[...], axis=0, keepdims=True) / feats
    for k in range(out_ref.shape[0]):
        out_ref[k, :kinds] = summed[pairs:]
        out_ref[k, kinds, 0:1] = square
        out_ref[k, kinds, 1:2] = loss


def sum_kernel(parts_ref, out_ref):
    summed = parts_ref[0]
    for k in range(1, parts_ref.shape[0]):
        summed = summed + parts_ref[k]
    out_ref[...] = summed


def pack_kernel(summed_ref, own_ref, other_ref, out_ref):
    kinds = summed_ref.shape[0] - 1
    pairs = own_ref.shape[0]
    model_grad, sums = summed_ref[:kinds], summed_ref[kinds]
    flip = lax.axis_index(CORE) == 1
    own, other = own_ref[...], other_ref[...]
    at = 0
    for share in (jnp.where(flip, other, own), jnp.where(flip, own, other)):
        for i in range(pairs):
            out_ref[0, at : at + 2, :] = share[i]
            at += 2
    for i in range(kinds):
        out_ref[0, at : at + 2, :] = model_grad[i]
        at += 2
    square = jnp.sum(jnp.sum(model_grad * model_grad, axis=0), axis=0, keepdims=True)
    out_ref[0, at : at + 1, :] = sums[0:1] + square
    out_ref[0, at + 1 : at + 2, :] = sums[1:2]
    if at + 2 < out_ref.shape[1]:
        out_ref[0, at + 2 :, :] = jnp.zeros((out_ref.shape[1] - at - 2, LANES), F32)
    packed = out_ref[0]
    for k in range(1, out_ref.shape[0]):
        out_ref[k] = packed


def final_kernel(share, kinds, parts_ref, proj_ref, models_ref, loss_ref):
    count = parts_ref.shape[0]
    sums = parts_ref[0, 2 * share :, :]
    for k in range(1, count):
        sums = sums + parts_ref[k, 2 * share :, :]
    sums = jnp.sum(sums, axis=1, keepdims=True)
    square, loss = (sums[kinds + i : kinds + i + 1] for i in range(2))
    loss_ref[...] = loss
    scale = jnp.sqrt(F32(D * R + NM * R)) / (jnp.sqrt(square) + 1e-06)
    for k in range(count):
        for c in range(2):
            to = (c * count + k) * share
            proj_ref[to : to + share, :] = scale * parts_ref[k, c * share : (c + 1) * share, :]
        models_ref[k * kinds : (k + 1) * kinds, :] = scale * parts_ref[k, 2 * share : 2 * share + kinds, :]


VMEM = pl.BlockSpec(memory_space=pltpu.VMEM)
HBM = pl.BlockSpec(memory_space=pltpu.HBM)


def kernel_call(body, outs, ins, limit, cost, in_specs=None, scratch=()):
    flops, moved = cost
    return pl.pallas_call(
        body,
        out_shape=outs,
        in_specs=in_specs or [VMEM] * len(ins),
        out_specs=jax.tree.map(lambda _: VMEM, outs),
        scratch_shapes=scratch,
        compiler_params=pltpu.CompilerParams(vmem_limit_bytes=limit * MIB),
        cost_estimate=pl.CostEstimate(flops=flops, bytes_accessed=moved, transcendentals=0),
    )(*ins)


def shape(*dims, kind=F32):
    return jax.ShapeDtypeStruct(dims, kind)


def body(queries, projection, models, first, second, wins):
    tokens, width = queries.shape
    rows, chips, feats = lax.axis_size(ROWS), lax.axis_size(CHIPS), lax.axis_size("feat")
    share = width // rows
    kinds = NM // chips
    first, second, wins = (x.reshape(tokens // LANES, LANES) for x in (first, second, wins))
    sources = (first, second, models, projection, queries)
    margins, held, gap, pick, proj = kernel_call(
        margin_kernel,
        (
            shape(feats, tokens // LANES, LANES),
            pltpu.VMEM((tokens, width), BF16),
            pltpu.VMEM((R, tokens), F32),
            pltpu.VMEM((NM, tokens), BF16),
            pltpu.VMEM(projection.shape, BF16),
        ),
        [pltpu.with_memory_space_constraint(x, pltpu.HBM) for x in sources],
        24,
        (2 * tokens * width * R, tokens * width * 2),
        in_specs=[HBM] * len(sources),
        scratch=[
            pltpu.VMEM(first.shape, jnp.int32),
            pltpu.VMEM(first.shape, jnp.int32),
            pltpu.VMEM(models.shape, F32),
            pltpu.SemaphoreType.DMA((tokens // BLOCK,)),
            pltpu.SemaphoreType.DMA((4,)),
        ],
    )
    margins = exchange(margins, "feat")
    half = shape(chips, share // 2, 2, LANES)
    other, loss, left, weighted = kernel_call(
        functools.partial(other_kernel, float(tokens * rows)),
        (
            half,
            shape(tokens // LANES, LANES),
            pltpu.VMEM((R + 2 * NM, tokens), BF16),
            pltpu.VMEM((NM, width // 2), F32),
        ),
        (margins, wins, gap, pick, held),
        24,
        (2 * tokens * width * R, tokens * width * 2),
        scratch=[pltpu.VMEM((tokens // LANES, LANES), F32), pltpu.VMEM((R + 2 * NM, width // 2), F32)],
    )
    other = swap(other)
    own, model_grad = kernel_call(
        own_kernel,
        (half, shape(chips, kinds // 2, 2, LANES)),
        (left, weighted, proj, held),
        24,
        (2 * tokens * width * R, tokens * width * 2),
    )
    parts = kernel_call(
        join_kernel, shape(chips, (share + kinds) // 2, 2, LANES), (own, other, model_grad), 4, (10000, 400000)
    )
    parts = exchange(parts, CHIPS)
    grad_share, parts = kernel_call(
        functools.partial(share_kernel, float(feats)),
        (shape(share // 2, 2, LANES), shape(2 * feats, kinds // 2 + 1, 2, LANES)),
        (parts, loss),
        4,
        (10000, 400000),
    )
    other_share = swap(grad_share)
    parts = exchange(parts, (CORE, "feat"))
    parts = kernel_call(sum_kernel, shape(*parts.shape[1:]), (parts,), 4, (10000, 100000))
    length = 2 * share + kinds + 2
    parts = kernel_call(
        pack_kernel, shape(chips, length + -length % 8, LANES), (parts, grad_share, other_share), 4, (10000, 400000)
    )
    parts = exchange(parts, CHIPS)
    update_proj, update_models, loss = kernel_call(
        functools.partial(final_kernel, share, kinds),
        (shape(width, R), shape(NM, R), shape(1, 1)),
        (parts,),
        4,
        (10000, 600000),
    )
    return update_proj, update_models, loss.reshape(())


def solution(mesh):
    split = Mesh(
        mesh.devices.reshape(4, 4, 2, mesh.shape["feat"]), ("rows_0", "rows_1", "rows_2", "feat")
    )
    in_specs = (P(ROWS, "feat"), P("feat", None), P(), P(ROWS), P(ROWS), P(ROWS))
    out_specs = (P("feat", None), P(), P())
    return jax.shard_map(body, mesh=split, in_specs=in_specs, out_specs=out_specs, check_vma=False)
```

```python
import functools

import jax
import jax.numpy as jnp
from jax import lax
from jax.experimental import pallas as pl
from jax.experimental.pallas import tpu as pltpu
from jax.sharding import Mesh
from jax.sharding import PartitionSpec as P


D = 4096
R = 128
NM = 64
LANES = 128
CORE = "rows_2"
CHIPS = ("rows_0", "rows_1")
ROWS = (*CHIPS, CORE)
F32 = jnp.float32
BF16 = jnp.bfloat16
MIB = 1 << 20
BLOCK = 1536
AHEAD = 2


def exchange(x, axis):
    return lax.all_to_all(x, axis, split_axis=0, concat_axis=0, tiled=True)


def swap(x):
    return lax.ppermute(x, CORE, [(0, 1), (1, 0)])


def pieces(x, count):
    terms = []
    for _ in range(count):
        term = x.astype(BF16)
        terms.append(term)
        x = x - term.astype(F32)
    return terms


def contract(a, b, dim_a, dim_b):
    return lax.dot_general(a, b, (((dim_a,), (dim_b,)), ((), ())), preferred_element_type=F32)


def model_table(models):
    stacked = jnp.concatenate([term.astype(F32) for term in pieces(models, 3)], axis=0)
    return stacked.T.astype(BF16)


def picks(first_ref, second_ref, start, count):
    labels = lax.broadcasted_iota(jnp.int32, (NM, LANES), 0)
    tiles = []
    for i in range(start // LANES, (start + count) // LANES):
        one = jnp.where(labels == first_ref[i : i + 1, :], 1.0, 0.0)
        two = jnp.where(labels == second_ref[i : i + 1, :], 1.0, 0.0)
        tiles.append(one - two)
    return jnp.concatenate(tiles, axis=1)


def margin_kernel(first_hbm, second_hbm, models_hbm, proj_hbm, q_hbm, out_ref, q_ref, gap_ref, pick_ref, proj_ref, first_ref, second_ref, models_ref, q_sems, sems):
    tokens = q_ref.shape[0]
    small = [(models_hbm, models_ref), (first_hbm, first_ref), (second_hbm, second_ref), (proj_hbm, proj_ref)]
    small = [pltpu.make_async_copy(a, b, sems.at[i]) for i, (a, b) in enumerate(small)]
    for copy in small:
        copy.start()
    blocks = [pl.ds(i * BLOCK, BLOCK) for i in range(tokens // BLOCK)]
    copies = [pltpu.make_async_copy(q_hbm.at[rows, :], q_ref.at[rows, :], q_sems.at[i]) for i, rows in enumerate(blocks)]
    for copy in copies[:AHEAD]:
        copy.start()
    for copy in small[:3]:
        copy.wait()
    table = model_table(models_ref[...])
    started = AHEAD
    for start in range(0, tokens, BLOCK):
        cut = slice(start, start + BLOCK)
        pick = picks(first_ref, second_ref, start, BLOCK).astype(BF16)
        pick_ref[:, cut] = pick
        gap_ref[:, cut] = contract(table, jnp.concatenate([pick, pick, pick], axis=0), 1, 0)
        if start > 0 and started < len(copies):
            copies[started].start()
            started += 1
    small[3].wait()
    proj = proj_ref[...].astype(F32).T.astype(BF16)
    for start in range(0, tokens, BLOCK):
        copies[start // BLOCK].wait()
        routed = contract(proj, q_ref[start : start + BLOCK, :], 1, 1)
        margin = jnp.sum(routed * gap_ref[:, start : start + BLOCK], axis=0, keepdims=True)
        for j in range(BLOCK // LANES):
            row = margin[:, j * LANES : (j + 1) * LANES]
            for k in range(out_ref.shape[0]):
                out_ref[k, start // LANES + j : start // LANES + j + 1, :] = row


def put_pairs(ref, at, rows):
    count = ref.shape[0]
    pairs = rows.shape[0] // count // 2
    for j in range(count):
        for i in range(pairs):
            row = 2 * (j * pairs + i)
            ref[j, at + i] = rows[row : row + 2]


def columns(half, width):
    return pl.ds(pl.multiple_of(half * width, width), width)


def other_kernel(total, margins_ref, wins_ref, gap_ref, pick_ref, q_ref, out_ref, wrong_ref, left_ref, weighted_ref, coef_ref, acc_ref):
    tokens = q_ref.shape[0]
    width = acc_ref.shape[1]
    margin = margins_ref[0]
    for k in range(1, margins_ref.shape[0]):
        margin = margin + margins_ref[k]
    sign = 2.0 * wins_ref[...].astype(F32) - 1.0
    wrong = -sign * margin
    wrong_ref[...] = wrong
    coef_ref[...] = -sign * jax.nn.sigmoid(wrong) / total
    other = columns(1 - lax.axis_index(CORE), width)
    for start in range(0, tokens, BLOCK):
        cut = slice(start, start + BLOCK)
        row = start // LANES
        coef = jnp.concatenate([coef_ref[row + j : row + j + 1, :] for j in range(BLOCK // LANES)], axis=1)
        back = (coef * gap_ref[:, cut]).astype(BF16)
        left = jnp.concatenate([back, *pieces(coef * pick_ref[:, cut].astype(F32), 2)], axis=0)
        left_ref[:, cut] = left
        part = contract(left, q_ref[cut, other], 1, 0)
        if start == 0:
            acc_ref[...] = part
        else:
            acc_ref[...] += part
    put_pairs(out_ref, 0, acc_ref[:R, :].T)
    weighted_ref[...] = acc_ref[R : R + NM, :] + acc_ref[R + NM :, :]


def own_kernel(total, left_ref, weighted_ref, wrong_ref, proj_ref, q_ref, out_ref, models_ref, loss_ref):
    loss_ref[...] = jax.nn.softplus(wrong_ref[...]) / total
    width = weighted_ref.shape[1]
    core = lax.axis_index(CORE)
    acc = contract(left_ref[...], q_ref[:, columns(core, width)], 1, 0)
    put_pairs(out_ref, 0, acc[:R].T)
    model_grad = jnp.zeros((NM, R), F32)
    for half, weighted in ((core, acc[R : R + NM] + acc[R + NM :]), (1 - core, weighted_ref[...])):
        terms = contract(jnp.concatenate(pieces(weighted, 3), axis=0), proj_ref[columns(half, width), :], 1, 0)
        model_grad = model_grad + (terms[:NM] + terms[NM : 2 * NM] + terms[2 * NM :])
    put_pairs(models_ref, 0, model_grad)


def join_kernel(own_ref, other_ref, models_ref, out_ref):
    pairs = own_ref.shape[1]
    out_ref[:, :pairs] = own_ref[...] + other_ref[...]
    out_ref[:, pairs:] = models_ref[...]


def share_kernel(feats, parts_ref, loss_ref, share_ref, out_ref):
    summed = parts_ref[0]
    for k in range(1, parts_ref.shape[0]):
        summed = summed + parts_ref[k]
    pairs = share_ref.shape[0]
    kinds = summed.shape[0] - pairs
    grad = summed[:pairs]
    share_ref[...] = grad
    square = jnp.sum(jnp.sum(grad * grad, axis=0), axis=0, keepdims=True)
    loss = jnp.sum(loss_ref[...], axis=0, keepdims=True) / feats
    for k in range(out_ref.shape[0]):
        out_ref[k, :kinds] = summed[pairs:]
        out_ref[k, kinds, 0:1] = square
        out_ref[k, kinds, 1:2] = loss


def sum_kernel(parts_ref, out_ref):
    summed = parts_ref[0]
    for k in range(1, parts_ref.shape[0]):
        summed = summed + parts_ref[k]
    out_ref[...] = summed


def pack_kernel(summed_ref, own_ref, other_ref, out_ref):
    kinds = summed_ref.shape[0] - 1
    pairs = own_ref.shape[0]
    model_grad, sums = summed_ref[:kinds], summed_ref[kinds]
    flip = lax.axis_index(CORE) == 1
    own, other = own_ref[...], other_ref[...]
    at = 0
    for share in (jnp.where(flip, other, own), jnp.where(flip, own, other)):
        for i in range(pairs):
            out_ref[0, at : at + 2, :] = share[i]
            at += 2
    for i in range(kinds):
        out_ref[0, at : at + 2, :] = model_grad[i]
        at += 2
    square = jnp.sum(jnp.sum(model_grad * model_grad, axis=0), axis=0, keepdims=True)
    out_ref[0, at : at + 1, :] = sums[0:1] + square
    out_ref[0, at + 1 : at + 2, :] = sums[1:2]
    if at + 2 < out_ref.shape[1]:
        out_ref[0, at + 2 :, :] = jnp.zeros((out_ref.shape[1] - at - 2, LANES), F32)
    packed = out_ref[0]
    for k in range(1, out_ref.shape[0]):
        out_ref[k] = packed


def final_kernel(share, kinds, parts_ref, proj_ref, models_ref, loss_ref):
    count = parts_ref.shape[0]
    sums = parts_ref[0, 2 * share :, :]
    for k in range(1, count):
        sums = sums + parts_ref[k, 2 * share :, :]
    sums = jnp.sum(sums, axis=1, keepdims=True)
    square, loss = (sums[kinds + i : kinds + i + 1] for i in range(2))
    loss_ref[...] = loss
    scale = jnp.sqrt(F32(D * R + NM * R)) / (jnp.sqrt(square) + 1e-06)
    for k in range(count):
        for c in range(2):
            to = (c * count + k) * share
            proj_ref[to : to + share, :] = scale * parts_ref[k, c * share : (c + 1) * share, :]
        models_ref[k * kinds : (k + 1) * kinds, :] = scale * parts_ref[k, 2 * share : 2 * share + kinds, :]


VMEM = pl.BlockSpec(memory_space=pltpu.VMEM)
HBM = pl.BlockSpec(memory_space=pltpu.HBM)


def kernel_call(body, outs, ins, limit, cost, in_specs=None, scratch=()):
    flops, moved = cost
    return pl.pallas_call(
        body,
        out_shape=outs,
        in_specs=in_specs or [VMEM] * len(ins),
        out_specs=jax.tree.map(lambda _: VMEM, outs),
        scratch_shapes=scratch,
        compiler_params=pltpu.CompilerParams(vmem_limit_bytes=limit * MIB),
        cost_estimate=pl.CostEstimate(flops=flops, bytes_accessed=moved, transcendentals=0),
    )(*ins)


def shape(*dims, kind=F32):
    return jax.ShapeDtypeStruct(dims, kind)


def body(queries, projection, models, first, second, wins):
    tokens, width = queries.shape
    rows, chips, feats = lax.axis_size(ROWS), lax.axis_size(CHIPS), lax.axis_size("feat")
    share = width // rows
    kinds = NM // chips
    first, second, wins = (x.reshape(tokens // LANES, LANES) for x in (first, second, wins))
    sources = (first, second, models, projection, queries)
    margins, held, gap, pick, proj = kernel_call(
        margin_kernel,
        (
            shape(feats, tokens // LANES, LANES),
            pltpu.VMEM((tokens, width), BF16),
            pltpu.VMEM((R, tokens), F32),
            pltpu.VMEM((NM, tokens), BF16),
            pltpu.VMEM(projection.shape, BF16),
        ),
        [pltpu.with_memory_space_constraint(x, pltpu.HBM) for x in sources],
        24,
        (2 * tokens * width * R, tokens * width * 2),
        in_specs=[HBM] * len(sources),
        scratch=[
            pltpu.VMEM(first.shape, jnp.int32),
            pltpu.VMEM(first.shape, jnp.int32),
            pltpu.VMEM(models.shape, F32),
            pltpu.SemaphoreType.DMA((tokens // BLOCK,)),
            pltpu.SemaphoreType.DMA((4,)),
        ],
    )
    margins = exchange(margins, "feat")
    half = shape(chips, share // 2, 2, LANES)
    other, wrong, left, weighted = kernel_call(
        functools.partial(other_kernel, float(tokens * rows)),
        (
            half,
            shape(tokens // LANES, LANES),
            pltpu.VMEM((R + 2 * NM, tokens), BF16),
            pltpu.VMEM((NM, width // 2), F32),
        ),
        (margins, wins, gap, pick, held),
        24,
        (2 * tokens * width * R, tokens * width * 2),
        scratch=[pltpu.VMEM((tokens // LANES, LANES), F32), pltpu.VMEM((R + 2 * NM, width // 2), F32)],
    )
    other = swap(other)
    own, model_grad, loss = kernel_call(
        functools.partial(own_kernel, float(tokens * rows)),
        (half, shape(chips, kinds // 2, 2, LANES), shape(tokens // LANES, LANES)),
        (left, weighted, wrong, proj, held),
        24,
        (2 * tokens * width * R, tokens * width * 2),
    )
    parts = kernel_call(
        join_kernel, shape(chips, (share + kinds) // 2, 2, LANES), (own, other, model_grad), 4, (10000, 400000)
    )
    parts = exchange(parts, CHIPS)
    grad_share, parts = kernel_call(
        functools.partial(share_kernel, float(feats)),
        (shape(share // 2, 2, LANES), shape(2 * feats, kinds // 2 + 1, 2, LANES)),
        (parts, loss),
        4,
        (10000, 400000),
    )
    other_share = swap(grad_share)
    parts = exchange(parts, (CORE, "feat"))
    parts = kernel_call(sum_kernel, shape(*parts.shape[1:]), (parts,), 4, (10000, 100000))
    length = 2 * share + kinds + 2
    parts = kernel_call(
        pack_kernel, shape(chips, length + -length % 8, LANES), (parts, grad_share, other_share), 4, (10000, 400000)
    )
    parts = exchange(parts, CHIPS)
    update_proj, update_models, loss = kernel_call(
        functools.partial(final_kernel, share, kinds),
        (shape(width, R), shape(NM, R), shape(1, 1)),
        (parts,),
        4,
        (10000, 600000),
    )
    return update_proj, update_models, loss.reshape(())


def solution(mesh):
    split = Mesh(
        mesh.devices.reshape(4, 4, 2, mesh.shape["feat"]), ("rows_0", "rows_1", "rows_2", "feat")
    )
    in_specs = (P(ROWS, "feat"), P("feat", None), P(), P(ROWS), P(ROWS), P(ROWS))
    out_specs = (P("feat", None), P(), P())
    return jax.shard_map(body, mesh=split, in_specs=in_specs, out_specs=out_specs, check_vma=False)
```

```python
import functools

import jax
import jax.numpy as jnp
from jax import lax
from jax.experimental import pallas as pl
from jax.experimental.pallas import tpu as pltpu
from jax.sharding import Mesh
from jax.sharding import PartitionSpec as P


D = 4096
R = 128
NM = 64
LANES = 128
CORE = "rows_2"
CHIPS = ("rows_0", "rows_1")
ROWS = (*CHIPS, CORE)
F32 = jnp.float32
BF16 = jnp.bfloat16
MIB = 1 << 20
BLOCK = 1536
AHEAD = 2
GAPS = 3072


def exchange(x, axis):
    return lax.all_to_all(x, axis, split_axis=0, concat_axis=0, tiled=True)


def swap(x):
    return lax.ppermute(x, CORE, [(0, 1), (1, 0)])


def pieces(x, count):
    terms = []
    for _ in range(count):
        term = x.astype(BF16)
        terms.append(term)
        x = x - term.astype(F32)
    return terms


def contract(a, b, dim_a, dim_b):
    return lax.dot_general(a, b, (((dim_a,), (dim_b,)), ((), ())), preferred_element_type=F32)


def model_table(models):
    stacked = jnp.concatenate([term.astype(F32) for term in pieces(models, 3)], axis=0)
    return stacked.T.astype(BF16)


def picks(first_ref, second_ref, start, count):
    labels = lax.broadcasted_iota(jnp.int32, (NM, LANES), 0)
    tiles = []
    for i in range(start // LANES, (start + count) // LANES):
        one = jnp.where(labels == first_ref[i : i + 1, :], 1.0, 0.0)
        two = jnp.where(labels == second_ref[i : i + 1, :], 1.0, 0.0)
        tiles.append(one - two)
    return jnp.concatenate(tiles, axis=1)


def margin_kernel(first_hbm, second_hbm, models_hbm, proj_hbm, q_hbm, out_ref, q_ref, gap_ref, pick_ref, proj_ref, first_ref, second_ref, models_ref, q_sems, sems):
    tokens = q_ref.shape[0]
    small = [(models_hbm, models_ref), (first_hbm, first_ref), (second_hbm, second_ref), (proj_hbm, proj_ref)]
    small = [pltpu.make_async_copy(a, b, sems.at[i]) for i, (a, b) in enumerate(small)]
    for copy in small:
        copy.start()
    blocks = [pl.ds(i * BLOCK, BLOCK) for i in range(tokens // BLOCK)]
    copies = [pltpu.make_async_copy(q_hbm.at[rows, :], q_ref.at[rows, :], q_sems.at[i]) for i, rows in enumerate(blocks)]
    for copy in copies[:AHEAD]:
        copy.start()
    for copy in small[:3]:
        copy.wait()
    table = model_table(models_ref[...])
    started = AHEAD
    for start in range(0, tokens, GAPS):
        cut = slice(start, start + GAPS)
        pick = picks(first_ref, second_ref, start, GAPS).astype(BF16)
        pick_ref[:, cut] = pick
        gap_ref[:, cut] = contract(table, jnp.concatenate([pick, pick, pick], axis=0), 1, 0)
        if started < len(copies):
            copies[started].start()
            started += 1
    for copy in copies[started:]:
        copy.start()
    small[3].wait()
    proj = proj_ref[...].astype(F32).T.astype(BF16)
    for start in range(0, tokens, BLOCK):
        copies[start // BLOCK].wait()
        routed = contract(proj, q_ref[start : start + BLOCK, :], 1, 1)
        margin = jnp.sum(routed * gap_ref[:, start : start + BLOCK], axis=0, keepdims=True)
        for j in range(BLOCK // LANES):
            row = margin[:, j * LANES : (j + 1) * LANES]
            for k in range(out_ref.shape[0]):
                out_ref[k, start // LANES + j : start // LANES + j + 1, :] = row


def put_pairs(ref, at, rows):
    count = ref.shape[0]
    pairs = rows.shape[0] // count // 2
    for j in range(count):
        for i in range(pairs):
            row = 2 * (j * pairs + i)
            ref[j, at + i] = rows[row : row + 2]


def columns(half, width):
    return pl.ds(pl.multiple_of(half * width, width), width)


def other_kernel(total, margins_ref, wins_ref, gap_ref, pick_ref, q_ref, out_ref, wrong_ref, left_ref, weighted_ref, coef_ref, acc_ref):
    tokens = q_ref.shape[0]
    width = acc_ref.shape[1]
    margin = margins_ref[0]
    for k in range(1, margins_ref.shape[0]):
        margin = margin + margins_ref[k]
    sign = 2.0 * wins_ref[...].astype(F32) - 1.0
    wrong = -sign * margin
    wrong_ref[...] = wrong
    coef_ref[...] = -sign * jax.nn.sigmoid(wrong) / total
    other = columns(1 - lax.axis_index(CORE), width)
    for start in range(0, tokens, BLOCK):
        cut = slice(start, start + BLOCK)
        row = start // LANES
        coef = jnp.concatenate([coef_ref[row + j : row + j + 1, :] for j in range(BLOCK // LANES)], axis=1)
        back = (coef * gap_ref[:, cut]).astype(BF16)
        left = jnp.concatenate([back, *pieces(coef * pick_ref[:, cut].astype(F32), 2)], axis=0)
        left_ref[:, cut] = left
        part = contract(left, q_ref[cut, other], 1, 0)
        if start == 0:
            acc_ref[...] = part
        else:
            acc_ref[...] += part
    put_pairs(out_ref, 0, acc_ref[:R, :].T)
    weighted_ref[...] = acc_ref[R : R + NM, :] + acc_ref[R + NM :, :]


def own_kernel(total, left_ref, weighted_ref, wrong_ref, proj_ref, q_ref, out_ref, models_ref, loss_ref):
    loss_ref[...] = jax.nn.softplus(wrong_ref[...]) / total
    width = weighted_ref.shape[1]
    core = lax.axis_index(CORE)
    acc = contract(left_ref[...], q_ref[:, columns(core, width)], 1, 0)
    put_pairs(out_ref, 0, acc[:R].T)
    model_grad = jnp.zeros((NM, R), F32)
    for half, weighted in ((core, acc[R : R + NM] + acc[R + NM :]), (1 - core, weighted_ref[...])):
        terms = contract(jnp.concatenate(pieces(weighted, 3), axis=0), proj_ref[columns(half, width), :], 1, 0)
        model_grad = model_grad + (terms[:NM] + terms[NM : 2 * NM] + terms[2 * NM :])
    put_pairs(models_ref, 0, model_grad)


def join_kernel(own_ref, other_ref, models_ref, out_ref):
    pairs = own_ref.shape[1]
    out_ref[:, :pairs] = own_ref[...] + other_ref[...]
    out_ref[:, pairs:] = models_ref[...]


def share_kernel(feats, parts_ref, loss_ref, share_ref, out_ref):
    summed = parts_ref[0]
    for k in range(1, parts_ref.shape[0]):
        summed = summed + parts_ref[k]
    pairs = share_ref.shape[0]
    kinds = summed.shape[0] - pairs
    grad = summed[:pairs]
    share_ref[...] = grad
    square = jnp.sum(jnp.sum(grad * grad, axis=0), axis=0, keepdims=True)
    loss = jnp.sum(loss_ref[...], axis=0, keepdims=True) / feats
    for k in range(out_ref.shape[0]):
        out_ref[k, :kinds] = summed[pairs:]
        out_ref[k, kinds, 0:1] = square
        out_ref[k, kinds, 1:2] = loss


def sum_kernel(parts_ref, out_ref):
    summed = parts_ref[0]
    for k in range(1, parts_ref.shape[0]):
        summed = summed + parts_ref[k]
    out_ref[...] = summed


def pack_kernel(summed_ref, own_ref, other_ref, out_ref):
    kinds = summed_ref.shape[0] - 1
    pairs = own_ref.shape[0]
    model_grad, sums = summed_ref[:kinds], summed_ref[kinds]
    flip = lax.axis_index(CORE) == 1
    own, other = own_ref[...], other_ref[...]
    at = 0
    for share in (jnp.where(flip, other, own), jnp.where(flip, own, other)):
        for i in range(pairs):
            out_ref[0, at : at + 2, :] = share[i]
            at += 2
    for i in range(kinds):
        out_ref[0, at : at + 2, :] = model_grad[i]
        at += 2
    square = jnp.sum(jnp.sum(model_grad * model_grad, axis=0), axis=0, keepdims=True)
    out_ref[0, at : at + 1, :] = sums[0:1] + square
    out_ref[0, at + 1 : at + 2, :] = sums[1:2]
    if at + 2 < out_ref.shape[1]:
        out_ref[0, at + 2 :, :] = jnp.zeros((out_ref.shape[1] - at - 2, LANES), F32)
    packed = out_ref[0]
    for k in range(1, out_ref.shape[0]):
        out_ref[k] = packed


def final_kernel(share, kinds, parts_ref, proj_ref, models_ref, loss_ref):
    count = parts_ref.shape[0]
    sums = parts_ref[0, 2 * share :, :]
    for k in range(1, count):
        sums = sums + parts_ref[k, 2 * share :, :]
    sums = jnp.sum(sums, axis=1, keepdims=True)
    square, loss = (sums[kinds + i : kinds + i + 1] for i in range(2))
    loss_ref[...] = loss
    scale = jnp.sqrt(F32(D * R + NM * R)) / (jnp.sqrt(square) + 1e-06)
    for k in range(count):
        for c in range(2):
            to = (c * count + k) * share
            proj_ref[to : to + share, :] = scale * parts_ref[k, c * share : (c + 1) * share, :]
        models_ref[k * kinds : (k + 1) * kinds, :] = scale * parts_ref[k, 2 * share : 2 * share + kinds, :]


VMEM = pl.BlockSpec(memory_space=pltpu.VMEM)
HBM = pl.BlockSpec(memory_space=pltpu.HBM)


def kernel_call(body, outs, ins, limit, cost, in_specs=None, scratch=()):
    flops, moved = cost
    return pl.pallas_call(
        body,
        out_shape=outs,
        in_specs=in_specs or [VMEM] * len(ins),
        out_specs=jax.tree.map(lambda _: VMEM, outs),
        scratch_shapes=scratch,
        compiler_params=pltpu.CompilerParams(vmem_limit_bytes=limit * MIB),
        cost_estimate=pl.CostEstimate(flops=flops, bytes_accessed=moved, transcendentals=0),
    )(*ins)


def shape(*dims, kind=F32):
    return jax.ShapeDtypeStruct(dims, kind)


def body(queries, projection, models, first, second, wins):
    tokens, width = queries.shape
    rows, chips, feats = lax.axis_size(ROWS), lax.axis_size(CHIPS), lax.axis_size("feat")
    share = width // rows
    kinds = NM // chips
    first, second, wins = (x.reshape(tokens // LANES, LANES) for x in (first, second, wins))
    sources = (first, second, models, projection, queries)
    margins, held, gap, pick, proj = kernel_call(
        margin_kernel,
        (
            shape(feats, tokens // LANES, LANES),
            pltpu.VMEM((tokens, width), BF16),
            pltpu.VMEM((R, tokens), F32),
            pltpu.VMEM((NM, tokens), BF16),
            pltpu.VMEM(projection.shape, BF16),
        ),
        [pltpu.with_memory_space_constraint(x, pltpu.HBM) for x in sources],
        24,
        (2 * tokens * width * R, tokens * width * 2),
        in_specs=[HBM] * len(sources),
        scratch=[
            pltpu.VMEM(first.shape, jnp.int32),
            pltpu.VMEM(first.shape, jnp.int32),
            pltpu.VMEM(models.shape, F32),
            pltpu.SemaphoreType.DMA((tokens // BLOCK,)),
            pltpu.SemaphoreType.DMA((4,)),
        ],
    )
    margins = exchange(margins, "feat")
    half = shape(chips, share // 2, 2, LANES)
    other, wrong, left, weighted = kernel_call(
        functools.partial(other_kernel, float(tokens * rows)),
        (
            half,
            shape(tokens // LANES, LANES),
            pltpu.VMEM((R + 2 * NM, tokens), BF16),
            pltpu.VMEM((NM, width // 2), F32),
        ),
        (margins, wins, gap, pick, held),
        24,
        (2 * tokens * width * R, tokens * width * 2),
        scratch=[pltpu.VMEM((tokens // LANES, LANES), F32), pltpu.VMEM((R + 2 * NM, width // 2), F32)],
    )
    other = swap(other)
    own, model_grad, loss = kernel_call(
        functools.partial(own_kernel, float(tokens * rows)),
        (half, shape(chips, kinds // 2, 2, LANES), shape(tokens // LANES, LANES)),
        (left, weighted, wrong, proj, held),
        24,
        (2 * tokens * width * R, tokens * width * 2),
    )
    parts = kernel_call(
        join_kernel, shape(chips, (share + kinds) // 2, 2, LANES), (own, other, model_grad), 4, (10000, 400000)
    )
    parts = exchange(parts, CHIPS)
    grad_share, parts = kernel_call(
        functools.partial(share_kernel, float(feats)),
        (shape(share // 2, 2, LANES), shape(2 * feats, kinds // 2 + 1, 2, LANES)),
        (parts, loss),
        4,
        (10000, 400000),
    )
    other_share = swap(grad_share)
    parts = exchange(parts, (CORE, "feat"))
    parts = kernel_call(sum_kernel, shape(*parts.shape[1:]), (parts,), 4, (10000, 100000))
    length = 2 * share + kinds + 2
    parts = kernel_call(
        pack_kernel, shape(chips, length + -length % 8, LANES), (parts, grad_share, other_share), 4, (10000, 400000)
    )
    parts = exchange(parts, CHIPS)
    update_proj, update_models, loss = kernel_call(
        functools.partial(final_kernel, share, kinds),
        (shape(width, R), shape(NM, R), shape(1, 1)),
        (parts,),
        4,
        (10000, 600000),
    )
    return update_proj, update_models, loss.reshape(())


def solution(mesh):
    split = Mesh(
        mesh.devices.reshape(4, 4, 2, mesh.shape["feat"]), ("rows_0", "rows_1", "rows_2", "feat")
    )
    in_specs = (P(ROWS, "feat"), P("feat", None), P(), P(ROWS), P(ROWS), P(ROWS))
    out_specs = (P("feat", None), P(), P())
    return jax.shard_map(body, mesh=split, in_specs=in_specs, out_specs=out_specs, check_vma=False)
```
